32 devices in a mesh: space: 8 (over z, x), tpair: 4 (over y, core).
Axes of the slice: x: 2, y: 2, z: 4, core: 2. Of those that a mesh axis runs over, the one named last changes fastest.
Arguments:
- eigvecs: bfloat16 [4, 2, 3, 64, 1024], P('tpair', None, None, None, 'space'), may hold values from -6 to 6
- momenta: int32 [8, 3], replicated, may hold values from -2 to 2
- perams: bfloat16 [4, 4, 16, 2, 4096], P('tpair'), may hold values from -0.5 to 0.5
- sources: int32 [4], replicated, may hold values from 0 to 3, each once
- spins: int32 [2, 3, 2], replicated, may hold values from 0 to 3
Outputs:
- baryon: float32 [4, 4, 2, 512, 2, 4096], P('tpair', None, None, 'space')
The draws below stay inside these ranges and needn't reach their ends.
Inputs may be any that keep to these rules, and one draw needn't show every extreme that they name: The entries of sources are distinct.
All inputs are finite; a program needn't handle non-finite values.
Results may differ from the reference program's by a relative error of at most 0.0064.
Values may be sent and summed in bfloat16 or wider, within the bound.
No kernel may reach another device: no remote copies, remote signals or barrier semaphores. Data moves between devices by JAX's collectives and lax.ppermute only.
A program may use at most 128 MiB of HBM per device.

```python
import jax
import jax.numpy as jnp
import numpy as np
from jax import lax

NVEC = 64
MOM = 8
LEXT = 64
NCOMB = 2
NSRC = 4
SITES_DEV = 128
NT = 4
SITES = 1024
N_SPACE = 8


def touch_ends(array, stream_key, low, top_value):
    extent = array.shape
    place = [jax.random.randint(jax.random.fold_in(stream_key, axis), (), 0, extent[axis]) for axis in range(len(extent))]
    array = array.at[tuple(place)].set(low)
    longest = extent.index(max(extent))
    place[longest] = (place[longest] + 1) % extent[longest]
    return array.at[tuple(place)].set(top_value)


def steps_of(key, extent, shards, smallest, high):
    factor_of, own = 1.0, jax.random.fold_in(key, 6)
    for dim, blocks in shards:
        heights = jnp.exp(jax.random.uniform(jax.random.fold_in(own, dim), (blocks,), jnp.float32, smallest / len(shards), high / len(shards)))
        factor_of = factor_of * jnp.repeat(heights, extent[dim] // blocks).reshape([-1 if axis == dim else 1 for axis in range(len(extent))])
    return factor_of


def centred(stream_key, extent, deviation, limit, shards=(), kind=jnp.bfloat16):
    values = deviation * jax.random.normal(stream_key, extent, jnp.float32)
    if shards:
        values = values * steps_of(stream_key, extent, shards, -0.22, 0.18)
    return jnp.clip(values, -limit, limit).astype(kind)


def setup_inputs(seed: int = 0) -> dict:
    streams_of = jax.random.split(jax.random.key(seed), 6)
    eigvecs = centred(streams_of[0], (NT, 2, 3, NVEC, SITES), 1.0, 6.0, ((0, 4), (4, 8)))
    momenta = touch_ends(jax.random.randint(streams_of[1], (MOM, 3), -2, 3), jax.random.fold_in(streams_of[1], 1), -2, 2).astype(jnp.int32)
    perams = centred(streams_of[2], (NT, NT, 16, 2, NVEC * NVEC), (2 * NVEC) ** -0.5, 0.5, ((0, 4),))
    sources = jax.random.permutation(streams_of[3], NT).astype(jnp.int32)
    spins = touch_ends(jax.random.randint(streams_of[4], (NCOMB, 3, 2), 0, 4), jax.random.fold_in(streams_of[4], 1), 0, 3).astype(jnp.int32)
    return dict(eigvecs=eigvecs, momenta=momenta, perams=perams, sources=sources, spins=spins)


TWO_PI = 6.283185307179586

def pair_tables(vectors):
    upper_rows, upper_cols = np.triu_indices(vectors, 1)
    total_pairs = vectors * vectors // 2
    left_index = np.zeros(total_pairs, np.int32)
    right_index = np.zeros(total_pairs, np.int32)
    left_index[:upper_rows.size] = upper_rows
    right_index[:upper_rows.size] = upper_cols
    position = np.zeros(vectors * vectors, np.int32)
    sign_table = np.zeros(vectors * vectors, np.float32)
    slot_ids = np.arange(upper_rows.size, dtype=np.int32)
    position[upper_rows * vectors + upper_cols] = slot_ids
    sign_table[upper_rows * vectors + upper_cols] = 1.0
    position[upper_cols * vectors + upper_rows] = slot_ids
    sign_table[upper_cols * vectors + upper_rows] = -1.0
    return (left_index, right_index, position, sign_table)

def cross_columns(left_vec, right_vec):
    left_f = left_vec.astype(jnp.float32)
    right_f = right_vec.astype(jnp.float32)
    pieces = []
    for colour in range(3):
        next_one = (colour + 1) % 3
        after_one = (colour + 2) % 3
        real_part = left_f[:, 0, next_one] * right_f[:, 0, after_one] - left_f[:, 1, next_one] * right_f[:, 1, after_one] - (left_f[:, 0, after_one] * right_f[:, 0, next_one] - left_f[:, 1, after_one] * right_f[:, 1, next_one])
        imag_part = left_f[:, 0, next_one] * right_f[:, 1, after_one] + left_f[:, 1, next_one] * right_f[:, 0, after_one] - (left_f[:, 0, after_one] * right_f[:, 1, next_one] + left_f[:, 1, after_one] * right_f[:, 0, next_one])
        pieces.append(jnp.stack([real_part, imag_part], axis=1))
    return jnp.stack(pieces, axis=2).astype(jnp.bfloat16)

def projected_left(block_vecs, momenta, offset, total_sites):
    site_count = block_vecs.shape[-1]
    site_ids = offset + jnp.arange(site_count, dtype=jnp.int32)
    coords = jnp.stack([site_ids % LEXT, site_ids // LEXT % LEXT, site_ids // (LEXT * LEXT)])
    turns = jnp.mod(lax.optimization_barrier(jnp.sum(momenta[:, :, None] * coords[None, :, :], axis=1)), LEXT)
    angle = turns.astype(jnp.float32) * (TWO_PI / LEXT)
    factor = lax.rsqrt(jnp.float32(24.0 * total_sites))
    cosine = (jnp.cos(angle) * factor)[:, None, None, :]
    sine = (jnp.sin(angle) * factor)[:, None, None, :]
    vfloat = block_vecs.astype(jnp.float32)
    left_real = cosine * vfloat[0][None] + sine * vfloat[1][None]
    left_imag = cosine * vfloat[1][None] - sine * vfloat[0][None]
    upper_half = jnp.stack([left_real, left_imag], axis=0)
    lower_half = jnp.stack([-left_imag, left_real], axis=0)
    stacked = jnp.stack([upper_half, lower_half], axis=0)
    mom_count = momenta.shape[0]
    vectors = block_vecs.shape[2]
    stacked = jnp.transpose(stacked, (0, 3, 5, 1, 2, 4)).reshape(6 * site_count, 2 * mom_count * vectors)
    return stacked.astype(jnp.bfloat16)

def complex_blocks(blocks):
    tau_real = blocks[..., 0, :, :]
    tau_imag = blocks[..., 1, :, :]
    upper_half = jnp.stack([tau_real, tau_imag], axis=-2)
    lower_half = jnp.stack([-tau_imag, tau_real], axis=-2)
    return jnp.stack([upper_half, lower_half], axis=-4)

def select_blocks(sink_perams, sources, spins, vectors):
    count_times = sink_perams.shape[0]
    pick_time = (sources[:, None] == jnp.arange(count_times, dtype=jnp.int32)[None, :]).astype(jnp.float32)
    spin_code = spins[:, :, 0] * 4 + spins[:, :, 1]
    pick_spin = (spin_code[:, :, None] == jnp.arange(16, dtype=jnp.int32)).astype(jnp.float32)
    chosen = jnp.einsum('st,cqa,taxy->scqxy', pick_time, pick_spin, sink_perams.astype(jnp.float32))
    return chosen.astype(jnp.bfloat16).reshape(sources.shape[0] * spins.shape[0], 3, 2, vectors, vectors)

def reference(eigvecs, momenta, perams, sources, spins):
    left_index, right_index, position, sign_table = pair_tables(NVEC)
    signs = jnp.asarray(sign_table).astype(jnp.bfloat16)
    outputs = []
    for sink in range(NT):
        vecs = eigvecs[sink]

        def block(running, offset):
            block_vecs = lax.dynamic_slice_in_dim(vecs, offset, SITES_DEV, 3)
            turned = jnp.transpose(block_vecs, (2, 0, 1, 3))
            columns = cross_columns(turned[left_index], turned[right_index]).reshape(left_index.size, -1)
            projected = projected_left(block_vecs, momenta, offset, SITES)
            return (running + jnp.dot(columns, projected, preferred_element_type=jnp.float32), None)
        starts = jnp.arange(N_SPACE, dtype=jnp.int32) * SITES_DEV
        empty_sum = jnp.zeros((left_index.size, 2 * MOM * NVEC), jnp.float32)
        summed, _ = lax.scan(block, empty_sum, starts)
        rounded = summed.astype(jnp.bfloat16)
        rounded = (rounded[position] * signs[:, None]).reshape(NVEC * NVEC, 2, MOM, NVEC)
        blocks = select_blocks(perams[:, sink], sources, spins, NVEC)
        ymats = complex_blocks(blocks).astype(jnp.float32)
        spread = jnp.einsum('cwmi,swiox->somxc', rounded.astype(jnp.float32), ymats[:, 0]).astype(jnp.bfloat16)
        count_sc = spread.shape[0]
        spread = spread.reshape(count_sc, 2, MOM * NVEC, NVEC, NVEC).astype(jnp.float32)
        middle = jnp.einsum('swpjk,swkox->spjox', spread, ymats[:, 2]).astype(jnp.bfloat16)
        result = jnp.einsum('spjwk,swjox->spoxk', middle.astype(jnp.float32), ymats[:, 1])
        outputs.append(result.reshape(NSRC, NCOMB, MOM * NVEC, 2, NVEC * NVEC))
    return jnp.stack(outputs, axis=0)
```

```python
import functools

import jax
import jax.numpy as jnp
from jax import lax
from jax.experimental import pallas as pl
from jax.experimental.pallas import tpu as pltpu
from jax.sharding import PartitionSpec as P

LEXT = 64
TWO_PI = 6.283185307179586
LANES = 128
NT_DIMS = (((1,), (1,)), ((), ()))
NN_DIMS = (((1,), (0,)), ((), ()))


def phases(momenta, own_momentum, total_sites):
    site_ids = jnp.arange(total_sites, dtype=jnp.int32)
    row = lax.dynamic_index_in_dim(momenta, own_momentum, 0, keepdims=False)
    turns = jnp.mod(
        row[0] * (site_ids % LEXT)
        + row[1] * (site_ids // LEXT % LEXT)
        + row[2] * (site_ids // (LEXT * LEXT)),
        LEXT,
    )
    angle = turns.astype(jnp.float32) * (TWO_PI / LEXT)
    factor = lax.rsqrt(jnp.float32(24.0 * total_sites))
    both = jnp.stack([jnp.cos(angle) * factor, jnp.sin(angle) * factor], axis=0)
    return jnp.transpose(both.reshape(2, total_sites // LANES, LANES), (1, 0, 2))


def elemental_kernel(v_ref, ph_ref, out_ref, vd_ref, p_ref, x_ref, acc_ref, up_ref, low_ref):
    step = pl.program_id(0)
    vectors = v_ref.shape[3]
    half = vectors // 2
    per_chunk = x_ref.shape[0] // vectors

    @pl.when(step == 0)
    def _():
        acc_ref[...] = jnp.zeros_like(acc_ref)

    cosine = ph_ref[0, 0:1, :]
    sine = ph_ref[0, 1:2, :]
    for colour in range(3):
        real = v_ref[0, 0, colour].astype(jnp.float32)
        imag = v_ref[0, 1, colour].astype(jnp.float32)
        for slot, value in enumerate((real, imag, real + imag)):
            vd_ref[3 * slot + colour, 0:vectors, :] = value
            vd_ref[3 * slot + colour, vectors : 2 * vectors, :] = value
        p_real = cosine * real + sine * imag
        p_imag = cosine * imag - sine * real
        rows = (
            (p_real, -p_imag),
            (-p_imag, -p_real),
            (p_imag, p_real),
            (p_real, -p_imag),
        )
        for n, (left, right) in enumerate(rows):
            at = 2 * LANES * colour
            p_ref[n * vectors : (n + 1) * vectors, at : at + LANES] = left.astype(jnp.bfloat16)
            p_ref[n * vectors : (n + 1) * vectors, at + LANES : at + 2 * LANES] = right.astype(
                jnp.bfloat16
            )

    def chunk(index, carry):
        for u in range(per_chunk):
            shift = index * per_chunk + u + 1
            for block in range(vectors // 16):
                a = [vd_ref[n, 16 * block : 16 * block + 16, :] for n in range(9)]
                b = [vd_ref[n, pl.ds(shift + 16 * block, 16), :] for n in range(9)]
                at_row = u * vectors + 16 * block
                for colour in range(3):
                    up = (colour + 1) % 3
                    down = (colour + 2) % 3
                    one = a[up] * b[down] - a[down] * b[up]
                    two = a[3 + up] * b[3 + down] - a[3 + down] * b[3 + up]
                    three = a[6 + up] * b[6 + down] - a[6 + down] * b[6 + up]
                    at = 2 * LANES * colour
                    x_ref[at_row : at_row + 16, at : at + LANES] = (one - two).astype(jnp.bfloat16)
                    x_ref[at_row : at_row + 16, at + LANES : at + 2 * LANES] = (
                        three - (one + two)
                    ).astype(jnp.bfloat16)
        rows = x_ref.shape[0]
        start = pl.multiple_of(index * rows, rows)
        acc_ref[pl.ds(start, rows), :] += lax.dot_general(
            x_ref[...], p_ref[...], NT_DIMS, preferred_element_type=jnp.float32
        )
        return carry

    lax.fori_loop(0, half // per_chunk, chunk, 0)

    @pl.when(step == pl.num_programs(0) - 1)
    def _():
        def spread(index, carry):
            shift = index + 1
            for block in range(vectors // 8):
                start = pl.multiple_of(index * vectors + 8 * block, 8)
                for part in range(2):
                    value = acc_ref[pl.ds(start, 8), part * LANES : (part + 1) * LANES]
                    up_ref[part, pl.ds(8 * block * (2 * vectors + 1) + shift, 8, 2 * vectors + 1), :] = value
                    low_ref[
                        part, pl.ds(8 * block * (vectors + 1) + shift * vectors, 8, vectors + 1), :
                    ] = value
            return carry

        lax.fori_loop(0, half, spread, 0)

        def fold(j, carry):
            k = lax.broadcasted_iota(jnp.int32, (vectors, LANES), 0)
            wide = pl.multiple_of(j * 2 * vectors, vectors)
            narrow = pl.multiple_of(j * vectors, vectors)
            for part in range(2):
                near_up = up_ref[part, pl.ds(wide, vectors), :]
                far_up = up_ref[part, pl.ds(wide + vectors, vectors), :]
                near_low = low_ref[part, pl.ds(narrow, vectors), :]
                far_low = low_ref[part, pl.ds(narrow + vectors * vectors, vectors), :]
                above = jnp.where(k - j <= half, near_up, -far_low)
                below = jnp.where(j - k < half, -near_low, far_up)
                full = jnp.where(k > j, above, jnp.where(k < j, below, 0.0))
                out_ref[part, j] = full.astype(jnp.bfloat16)
            return carry

        lax.fori_loop(0, vectors, fold, 0)


def elementals(gathered, phase):
    owners, _, _, vectors, sites_here = gathered.shape
    per_owner = sites_here // LANES
    steps = owners * per_owner
    half = vectors // 2
    per_chunk = min(8, half)
    return pl.pallas_call(
        elemental_kernel,
        grid=(steps,),
        in_specs=[
            pl.BlockSpec(
                (1, 2, 3, vectors, LANES), lambda s: (s // per_owner, 0, 0, 0, s % per_owner)
            ),
            pl.BlockSpec((1, 2, LANES), lambda s: (s, 0, 0)),
        ],
        out_specs=pl.BlockSpec((2, vectors, vectors, 2 * vectors), lambda s: (0, 0, 0, 0)),
        out_shape=jax.ShapeDtypeStruct((2, vectors, vectors, 2 * vectors), jnp.bfloat16),
        scratch_shapes=[
            pltpu.VMEM((9, 2 * vectors, LANES), jnp.float32),
            pltpu.VMEM((4 * vectors, 6 * LANES), jnp.bfloat16),
            pltpu.VMEM((per_chunk * vectors, 6 * LANES), jnp.bfloat16),
            pltpu.VMEM((half * vectors, 4 * vectors), jnp.float32),
            pltpu.VMEM((2, 2 * vectors * vectors, LANES), jnp.float32),
            pltpu.VMEM((2, 2 * vectors * vectors, LANES), jnp.float32),
        ],
        compiler_params=pltpu.CompilerParams(
            dimension_semantics=("arbitrary",), vmem_limit_bytes=56 << 20
        ),
        cost_estimate=pl.CostEstimate(
            flops=2 * half * vectors * 6 * LANES * 4 * vectors * steps * 8,
            transcendentals=0,
            bytes_accessed=2 * gathered.size + 4 * vectors**3 * 2,
        ),
        name="elementals",
    )(gathered, phase)


def baryon_kernel(e_ref, l0_ref, t1_ref, w2_ref, out_ref, d_ref):
    step = pl.program_id(0)
    vectors = e_ref.shape[1]
    count = l0_ref.shape[0]
    rows_here = count // pl.num_programs(0)
    half = vectors // 2

    @pl.when(step == 0)
    def _():
        left = l0_ref[...]

        def one(j, carry):
            right = jnp.concatenate([e_ref[0, j], e_ref[1, j]], axis=0)
            value = lax.dot_general(left, right, NT_DIMS, preferred_element_type=jnp.float32)
            d_ref[pl.ds(j, count, vectors), :] = value
            return carry

        lax.fori_loop(0, vectors, one, 0, unroll=2)

    lanes = lax.broadcasted_iota(jnp.int32, (vectors, 2 * vectors), 1)
    left1 = t1_ref[0]
    right2 = w2_ref[0]
    group = 8

    def rows(index, carry):
        pieces = []
        for pair in range(group // 2):
            columns = []
            for one in range(2):
                row = (step * rows_here + index * group + 2 * pair + one) * vectors
                plain = d_ref[pl.ds(pl.multiple_of(row, vectors), vectors), :]
                turned = pltpu.roll(plain, vectors, 1)
                turned = jnp.where(lanes < vectors, -turned, turned)
                columns.append(
                    jnp.concatenate(
                        [plain.astype(jnp.bfloat16), turned.astype(jnp.bfloat16)], axis=0
                    )
                )
            right = jnp.concatenate(columns, axis=1)
            middle = lax.dot_general(left1, right, NN_DIMS, preferred_element_type=jnp.float32)
            middle = middle.astype(jnp.bfloat16)
            for one in range(2):
                at = one * 2 * vectors
                part = middle[:, at : at + 2 * vectors]
                pieces.append(jnp.concatenate([part[:half], part[half:]], axis=1))
        stacked = jnp.concatenate(pieces, axis=0)
        value = lax.dot_general(stacked, right2, NN_DIMS, preferred_element_type=jnp.float32)
        base = index * group * half * 2
        for part in range(2):
            out_ref[0, pl.ds(base + part, group * half, 2), :] = value[
                :, part * 2 * vectors : (part + 1) * 2 * vectors
            ]
        return carry

    lax.fori_loop(0, rows_here // group, rows, 0)


def baryons(elemental, l0, t1, w2):
    vectors = elemental.shape[1]
    count_sc = t1.shape[0]
    rows_here = l0.shape[0] // count_sc
    return pl.pallas_call(
        baryon_kernel,
        grid=(count_sc,),
        in_specs=[
            pl.BlockSpec(elemental.shape, lambda s: (0, 0, 0, 0)),
            pl.BlockSpec(l0.shape, lambda s: (0, 0)),
            pl.BlockSpec((1,) + t1.shape[1:], lambda s: (s, 0, 0)),
            pl.BlockSpec((1,) + w2.shape[1:], lambda s: (s, 0, 0)),
        ],
        out_specs=pl.BlockSpec((1, rows_here * vectors, 2 * vectors), lambda s: (s, 0, 0)),
        out_shape=jax.ShapeDtypeStruct(
            (count_sc, rows_here * vectors, 2 * vectors), jnp.float32
        ),
        scratch_shapes=[pltpu.VMEM((l0.shape[0] * vectors, 2 * vectors), jnp.float32)],
        compiler_params=pltpu.CompilerParams(
            dimension_semantics=("arbitrary",), vmem_limit_bytes=56 << 20
        ),
        name="baryons",
    )(elemental, l0, t1, w2)


def chosen_perams(perams, sources, spins):
    count_times = perams.shape[1]
    codes = (spins[:, :, 0] * 4 + spins[:, :, 1]).reshape(-1)
    local = perams[0]
    picked = jnp.stack(
        [
            lax.dynamic_index_in_dim(local, codes[n], 1, keepdims=False)
            for n in range(codes.shape[0])
        ],
        axis=1,
    )
    arrived = lax.all_to_all(picked, "tpair", split_axis=0, concat_axis=0, tiled=True)
    return jnp.stack(
        [
            lax.dynamic_index_in_dim(arrived, sources[s], 0, keepdims=False)
            for s in range(count_times)
        ],
        axis=0,
    )


def on_device(eigvecs, momenta, perams, sources, spins):
    vectors = eigvecs.shape[3]
    sites_here = eigvecs.shape[4]
    mom_count = momenta.shape[0]
    combos = spins.shape[0]
    space_count = lax.axis_size("space")
    place = lax.axis_index("space")
    rows_here = mom_count * vectors // space_count
    count_sc = sources.shape[0] * combos
    own_momentum = place * rows_here // vectors

    tau = chosen_perams(perams, sources, spins)
    tau = tau.reshape(count_sc, 3, 2, vectors, vectors)

    gathered = lax.all_gather(eigvecs[0], "space", axis=0, tiled=False)
    phase = phases(momenta, own_momentum, sites_here * space_count)
    elemental = elementals(gathered, phase)

    flipped = jnp.transpose(tau[:, :2], (0, 1, 4, 2, 3)).reshape(
        count_sc, 2, vectors, 2 * vectors
    )
    l0 = flipped[:, 0]
    if rows_here != vectors:
        l0 = lax.dynamic_slice_in_dim(l0, place * rows_here % vectors, rows_here, 1)
    l0 = l0.reshape(count_sc * rows_here, 2 * vectors)
    t1 = flipped[:, 1].reshape(count_sc, vectors // 2, 2, 2 * vectors)
    t1 = jnp.transpose(t1, (0, 2, 1, 3)).reshape(count_sc, vectors, 2 * vectors)
    real = tau[:, 2, 0]
    imag = tau[:, 2, 1]
    for_real = jnp.concatenate([real, -imag], axis=1)
    for_imag = jnp.concatenate([imag, real], axis=1)
    zero = jnp.zeros_like(for_real)
    w2 = jnp.concatenate(
        [
            jnp.concatenate([for_real, zero, for_imag, zero], axis=2),
            jnp.concatenate([zero, for_real, zero, for_imag], axis=2),
        ],
        axis=1,
    )
    result = baryons(elemental, l0, t1, w2)
    result = result.reshape(count_sc, rows_here, vectors // 2, 2, 2 * vectors)
    result = jnp.transpose(result, (0, 1, 3, 2, 4))
    return result.reshape(1, sources.shape[0], combos, rows_here, 2, vectors * vectors)


def solution(mesh):
    placed = (
        P("tpair", None, None, None, "space"),
        P(),
        P("tpair", None, None, None, None),
        P(),
        P(),
    )
    return jax.shard_map(
        on_device,
        mesh=mesh,
        in_specs=placed,
        out_specs=P("tpair", None, None, "space", None, None),
        check_vma=False,
    )
```

```python
import functools

import jax
import jax.numpy as jnp
from jax import lax
from jax.experimental import pallas as pl
from jax.experimental.pallas import tpu as pltpu
from jax.sharding import PartitionSpec as P

LEXT = 64
TWO_PI = 6.283185307179586
LANES = 128
NT_DIMS = (((1,), (1,)), ((), ()))
NN_DIMS = (((1,), (0,)), ((), ()))


def elemental_kernel(place_ref, mom_ref, *refs, first, parts, owners, sites_here, has_sum, last):
    inputs = refs[:parts]
    sum_ref = refs[parts] if has_sum else None
    refs = refs[parts + has_sum :]
    out_ref, v_ref, sem, vd_ref, p_ref, x0_ref, x1_ref = refs[:7]
    acc_ref, up_ref, low_ref = refs[7:] if last else (out_ref, None, None)
    vectors = v_ref.shape[3]
    half = vectors // 2
    rows = x0_ref.shape[0]
    per_chunk = rows // vectors
    chunks = half // per_chunk
    per_owner = sites_here // LANES
    blocks = v_ref.shape[0]

    copies = []
    for block in range(blocks):
        owner = block // per_owner
        ref = inputs[owner] if parts > 1 or owners == 1 else inputs[0].at[owner]
        at = block % per_owner * LANES
        copies.append(
            pltpu.make_async_copy(ref.at[:, :, :, at : at + LANES], v_ref.at[block], sem.at[block])
        )
    for copy in copies:
        copy.start()

    if has_sum and last:
        acc_ref[...] = sum_ref[...]
    elif not has_sum:
        acc_ref[...] = jnp.zeros_like(acc_ref)

    x1_ref[...] = jnp.zeros_like(x1_ref)
    p_ref[1] = jnp.zeros_like(p_ref[1])
    for copy in copies:
        copy.wait()
    lane = lax.broadcasted_iota(jnp.int32, (LANES, 2 * vectors), 1)
    total = place_ref[2]
    row = place_ref[1]
    factor = lax.rsqrt(jnp.full((1, LANES), 24.0, jnp.float32) * total.astype(jnp.float32))

    def one_block(block, unused):
        slot = block % 2
        owner = jnp.bitwise_xor(place_ref[0], first + block // per_owner)
        sites = (
            owner * sites_here
            + block % per_owner * LANES
            + lax.broadcasted_iota(jnp.int32, (1, LANES), 1)
        )
        turns = (
            mom_ref[row, 0] * jnp.bitwise_and(sites, LEXT - 1)
            + mom_ref[row, 1] * jnp.bitwise_and(sites // LEXT, LEXT - 1)
            + mom_ref[row, 2] * (sites // (LEXT * LEXT))
        )
        turns = jnp.bitwise_and(turns, LEXT - 1)
        angle = turns.astype(jnp.float32) * (TWO_PI / LEXT)
        cosine = jnp.cos(angle) * factor
        sine = jnp.sin(angle) * factor
        for colour in range(3):
            real = v_ref[block, 0, colour].astype(jnp.float32)
            imag = v_ref[block, 1, colour].astype(jnp.float32)
            for place, value in enumerate((real, imag, real + imag)):
                vd_ref[3 * place + colour, 0:vectors, :] = value
                vd_ref[3 * place + colour, vectors : 2 * vectors, :] = value
            p_real = cosine * real + sine * imag
            p_imag = cosine * imag - sine * real
            plain = jnp.transpose(jnp.concatenate([p_real, p_imag], axis=0))
            turned = pltpu.roll(plain, vectors, 1)
            signed = jnp.where(lane < vectors, plain, -plain)
            at = 2 * LANES * colour
            p_ref[slot, at : at + LANES, 0 : 2 * vectors] = signed.astype(jnp.bfloat16)
            p_ref[slot, at : at + LANES, 2 * vectors : 4 * vectors] = turned.astype(jnp.bfloat16)
            p_ref[slot, at + LANES : at + 2 * LANES, 0 : 2 * vectors] = (-turned).astype(
                jnp.bfloat16
            )
            p_ref[slot, at + LANES : at + 2 * LANES, 2 * vectors : 4 * vectors] = signed.astype(
                jnp.bfloat16
            )

        def cross(index, x_ref):
            for u in range(per_chunk):
                shift = index * per_chunk + u + 1
                for block in range(vectors // 16):
                    at_row = u * vectors + 16 * block
                    for colour in range(3):
                        up = (colour + 1) % 3
                        down = (colour + 2) % 3
                        reals = []
                        imags = []
                        for part in range(2):
                            row = 16 * block + 8 * part
                            parts = []
                            for place in range(3):
                                a_up = vd_ref[3 * place + up, row : row + 8, :]
                                a_down = vd_ref[3 * place + down, row : row + 8, :]
                                b_up = vd_ref[3 * place + up, pl.ds(shift + row, 8), :]
                                b_down = vd_ref[3 * place + down, pl.ds(shift + row, 8), :]
                                parts.append(a_up * b_down - a_down * b_up)
                            one, two, three = parts
                            reals.append(one - two)
                            imags.append(three - (one + two))
                        at = 2 * LANES * colour
                        x_ref[at_row : at_row + 16, at : at + LANES] = jnp.concatenate(
                            reals, axis=0
                        ).astype(jnp.bfloat16)
                        x_ref[at_row : at_row + 16, at + LANES : at + 2 * LANES] = jnp.concatenate(
                            imags, axis=0
                        ).astype(jnp.bfloat16)

        def add(index, x_ref, which):
            start = pl.multiple_of(index * rows, rows)
            acc_ref[pl.ds(start, rows), :] += lax.dot_general(
                x_ref[...], p_ref[which], NN_DIMS, preferred_element_type=jnp.float32
            )

        def two_chunks(index, carry):
            before = (2 * index + chunks - 1) % chunks
            cross(2 * index, x0_ref)
            add(before, x1_ref, jnp.where(index == 0, 1 - slot, slot))
            cross(2 * index + 1, x1_ref)
            add(2 * index, x0_ref, slot)
            return carry

        lax.fori_loop(0, chunks // 2, two_chunks, 0)
        return unused

    lax.fori_loop(0, blocks, one_block, 0)
    final = (blocks - 1) % 2
    start = (chunks - 1) * rows
    acc_ref[start : start + rows, :] += lax.dot_general(
        x1_ref[...], p_ref[final], NN_DIMS, preferred_element_type=jnp.float32
    )

    if last:

        def spread(index, carry):
            shift = index + 1
            for block in range(vectors // 8):
                start = pl.multiple_of(index * vectors + 8 * block, 8)
                for part in range(2):
                    value = acc_ref[pl.ds(start, 8), part * LANES : (part + 1) * LANES]
                    up_ref[part, pl.ds(8 * block * (2 * vectors + 1) + shift, 8, 2 * vectors + 1), :] = value
                    low_ref[
                        part, pl.ds(8 * block * (vectors + 1) + shift * vectors, 8, vectors + 1), :
                    ] = value
            return carry

        lax.fori_loop(0, half, spread, 0)

        def fold(j, carry):
            k = lax.broadcasted_iota(jnp.int32, (vectors, LANES), 0)
            wide = pl.multiple_of(j * 2 * vectors, vectors)
            narrow = pl.multiple_of(j * vectors, vectors)
            for part in range(2):
                near_up = up_ref[part, pl.ds(wide, vectors), :]
                far_up = up_ref[part, pl.ds(wide + vectors, vectors), :]
                near_low = low_ref[part, pl.ds(narrow, vectors), :]
                far_low = low_ref[part, pl.ds(narrow + vectors * vectors, vectors), :]
                above = jnp.where(k - j <= half, near_up, -far_low)
                below = jnp.where(j - k < half, -near_low, far_up)
                full = jnp.where(k > j, above, jnp.where(k < j, below, 0.0))
                out_ref[part, j] = full.astype(jnp.bfloat16)
            return carry

        lax.fori_loop(0, vectors, fold, 0)


def elementals(inputs, place, momenta, owners, first, running, last):
    vectors, sites_here = inputs[0].shape[-2:]
    half = vectors // 2
    per_chunk = half // 2
    parts = len(inputs)
    blocks = (parts if owners == 1 else owners) * sites_here // LANES
    sum_shape = (half * vectors, 4 * vectors)
    vmem = pl.BlockSpec(memory_space=pltpu.VMEM)
    smem = pl.BlockSpec(memory_space=pltpu.SMEM)
    has_sum = running is not None
    scratch = [
        pltpu.VMEM((blocks, 2, 3, vectors, LANES), jnp.bfloat16),
        pltpu.SemaphoreType.DMA((blocks,)),
        pltpu.VMEM((9, 2 * vectors, LANES), jnp.float32),
        pltpu.VMEM((2, 6 * LANES, 4 * vectors), jnp.bfloat16),
        pltpu.VMEM((per_chunk * vectors, 6 * LANES), jnp.bfloat16),
        pltpu.VMEM((per_chunk * vectors, 6 * LANES), jnp.bfloat16),
    ]
    if last:
        out_shape = jax.ShapeDtypeStruct((2, vectors, vectors, 2 * vectors), jnp.bfloat16)
        scratch += [
            pltpu.VMEM(sum_shape, jnp.float32),
            pltpu.VMEM((2, 2 * vectors * vectors, LANES), jnp.float32),
            pltpu.VMEM((2, 2 * vectors * vectors, LANES), jnp.float32),
        ]
    else:
        out_shape = jax.ShapeDtypeStruct(sum_shape, jnp.float32)
    return pl.pallas_call(
        functools.partial(
            elemental_kernel,
            first=first,
            parts=parts,
            owners=owners,
            sites_here=sites_here,
            has_sum=has_sum,
            last=last,
        ),
        in_specs=[smem, smem] + [pl.BlockSpec(memory_space=pl.ANY)] * parts + [vmem] * has_sum,
        out_specs=vmem,
        out_shape=out_shape,
        scratch_shapes=scratch,
        input_output_aliases={2 + parts: 0} if has_sum and not last else {},
        compiler_params=pltpu.CompilerParams(
            vmem_limit_bytes=(40 if last else 12) << 20
        ),
        cost_estimate=pl.CostEstimate(
            flops=blocks * 2 * half * vectors * 6 * LANES * 4 * vectors,
            transcendentals=0,
            bytes_accessed=blocks * 6 * vectors * LANES * 2,
        ),
        name="elementals",
    )(place, momenta, *inputs, *([running] if has_sum else []))


def select_kernel(sources_ref, spins_ref, tau_ref, out_ref):
    combos, quarks, _ = spins_ref.shape
    for s in range(sources_ref.shape[0]):
        for n in range(combos):
            for q in range(quarks):
                code = spins_ref[n, q, 0] * 4 + spins_ref[n, q, 1]
                out_ref[s * combos + n, q] = tau_ref[sources_ref[s], code]


def select(tau, sources, spins):
    smem = pl.BlockSpec(memory_space=pltpu.SMEM)
    vmem = pl.BlockSpec(memory_space=pltpu.VMEM)
    return pl.pallas_call(
        select_kernel,
        in_specs=[smem, smem, vmem],
        out_specs=vmem,
        out_shape=jax.ShapeDtypeStruct(
            (sources.shape[0] * spins.shape[0], spins.shape[1]) + tau.shape[2:], tau.dtype
        ),
        compiler_params=pltpu.CompilerParams(vmem_limit_bytes=4 << 20),
        name="select",
    )(sources, spins, tau)


def baryon_kernel(
    info_ref, e_ref, tau_ref, out_ref, d_ref, m_ref, l0_ref, t_ref, w2_ref
):
    step = pl.program_id(0)
    vectors = e_ref.shape[1]
    count_sc = pl.num_programs(0)
    half = vectors // 2
    count = l0_ref.shape[0]
    rows_here = count // count_sc
    pitch = vectors + 1

    def block(at, q, part):
        return tau_ref[at, q, part].astype(jnp.float32)

    def flipped(at, q):
        return jnp.transpose(jnp.concatenate([block(at, q, 0), block(at, q, 1)], axis=0))[:vectors]

    @pl.when(step == 0)
    def _():
        for at in range(tau_ref.shape[0]):
            t_ref[...] = flipped(at, 0)
            l0_ref[at * rows_here : (at + 1) * rows_here] = t_ref[pl.ds(info_ref[3], rows_here), :]
        w2_ref[...] = jnp.zeros_like(w2_ref)
        left = l0_ref[...].astype(jnp.bfloat16)

        def one(pair, carry):
            right = jnp.concatenate(
                [e_ref[part, 2 * pair + side] for side in range(2) for part in range(2)], axis=0
            )
            value = lax.dot_general(left, right, NT_DIMS, preferred_element_type=jnp.float32)
            for side in range(2):
                for row in range(count // 8):
                    d_ref[pl.ds(8 * row * pitch + 2 * pair + side, 8, pitch), :] = value[
                        8 * row : 8 * row + 8, side * 2 * vectors : (side + 1) * 2 * vectors
                    ]
            return carry

        lax.fori_loop(0, half, one, 0, unroll=2)

    t_ref[...] = flipped(step, 1)
    left1 = jnp.concatenate(
        [t_ref[pl.ds(low, half, 2), :] for low in range(2)], axis=0
    ).astype(jnp.bfloat16)
    real = block(step, 2, 0)
    imag = block(step, 2, 1)
    quarters = ((real, imag), (-imag, real))
    for part in range(2):
        for q in range(2):
            piece = quarters[part][q]
            for low in range(2):
                rows = (2 * low + part) * vectors
                w2_ref[rows : rows + vectors, 2 * q * vectors : 2 * (q + 1) * vectors] = (
                    pltpu.roll(piece, low * vectors, 1) if low else piece
                ).astype(jnp.bfloat16)

    lanes = lax.broadcasted_iota(jnp.int32, (vectors, 2 * vectors), 1)
    group = 8

    def rows(index, carry):
        for pair in range(group // 2):
            columns = []
            for one in range(2):
                row = (step * rows_here + index * group + 2 * pair + one) * pitch
                plain = d_ref[pl.ds(row, vectors), :]
                turned = pltpu.roll(plain, vectors, 1)
                turned = jnp.where(lanes < vectors, -turned, turned)
                columns.append(
                    jnp.concatenate(
                        [plain.astype(jnp.bfloat16), turned.astype(jnp.bfloat16)], axis=0
                    )
                )
            right = jnp.concatenate(columns, axis=1)
            middle = lax.dot_general(left1, right, NN_DIMS, preferred_element_type=jnp.float32)
            middle = middle.astype(jnp.bfloat16)
            for one in range(2):
                at = one * 2 * vectors
                base = pl.multiple_of(index * group * half, group * half) + (2 * pair + one) * half
                m_ref[pl.ds(base, half), 0 : 2 * vectors] = middle[:half, at : at + 2 * vectors]
                m_ref[pl.ds(base, half), 2 * vectors :] = middle[half:, at : at + 2 * vectors]
        return carry

    lax.fori_loop(0, rows_here // group, rows, 0, unroll=min(2, rows_here // group))
    value = lax.dot_general(m_ref[...], w2_ref[...], NN_DIMS, preferred_element_type=jnp.float32)
    for part in range(2):
        out_ref[0, pl.ds(part, rows_here * half, 2), :] = value[
            :, part * 2 * vectors : (part + 1) * 2 * vectors
        ]


def baryons(elemental, tau, info, rows_here):
    vectors = elemental.shape[1]
    count_sc = tau.shape[0]
    vmem = pl.BlockSpec(memory_space=pltpu.VMEM)
    smem = pl.BlockSpec(memory_space=pltpu.SMEM)
    return pl.pallas_call(
        baryon_kernel,
        grid=(count_sc,),
        in_specs=[smem, vmem, vmem],
        out_specs=pl.BlockSpec((1, rows_here * vectors, 2 * vectors), lambda s: (s, 0, 0)),
        out_shape=jax.ShapeDtypeStruct(
            (count_sc, rows_here * vectors, 2 * vectors), jnp.float32
        ),
        scratch_shapes=[
            pltpu.VMEM((count_sc * rows_here * (vectors + 1), 2 * vectors), jnp.float32),
            pltpu.VMEM((rows_here * vectors // 2, 4 * vectors), jnp.bfloat16),
            pltpu.VMEM((count_sc * rows_here, 2 * vectors), jnp.float32),
            pltpu.VMEM((vectors, 2 * vectors), jnp.float32),
            pltpu.VMEM((4 * vectors, 4 * vectors), jnp.bfloat16),
        ],
        compiler_params=pltpu.CompilerParams(
            dimension_semantics=("arbitrary",), vmem_limit_bytes=40 << 20
        ),
        name="baryons",
    )(info, elemental, tau)


GROUPS = ((0, 2), (2, 4), (4, 8))


def on_device(eigvecs, momenta, perams, sources, spins):
    vecs = eigvecs[0]
    vectors, sites_here = vecs.shape[2:]
    mom_count = momenta.shape[0]
    combos = spins.shape[0]
    space_count = lax.axis_size("space")
    place = lax.axis_index("space")
    rows_here = mom_count * vectors // space_count
    count_sc = sources.shape[0] * combos
    if vectors % rows_here or sites_here % LANES:
        raise ValueError("sizes")
    own_momentum = place * rows_here // vectors

    tau = lax.all_to_all(perams[0], "tpair", split_axis=0, concat_axis=0, tiled=True)

    by_permute = space_count == GROUPS[-1][-1]
    info = jnp.stack(
        [
            place if by_permute else 0 * place,
            own_momentum,
            0 * place + sites_here * space_count,
            place * rows_here % vectors,
        ]
    ).astype(jnp.int32)
    if by_permute:
        arrived = [vecs] + [
            lax.ppermute(vecs, "space", [(n, n ^ s) for n in range(space_count)])
            for s in range(1, space_count)
        ]
        running = None
        for begin, end in GROUPS:
            running = elementals(
                arrived[begin:end], info, momenta, 1, begin, running, end == space_count
            )
        elemental = running
    else:
        gathered = lax.all_gather(vecs, "space", axis=0, tiled=False)
        elemental = elementals([gathered], info, momenta, space_count, 0, None, True)

    tau = select(tau, sources, spins)
    tau = tau.reshape(tau.shape[:3] + (vectors, vectors))
    tau = jnp.pad(tau, ((0, 0),) * 4 + ((0, vectors),))
    result = baryons(elemental, tau, info, rows_here)
    result = result.reshape(count_sc, rows_here, vectors // 2, 2, 2 * vectors)
    result = jnp.transpose(result, (0, 1, 3, 2, 4))
    return result.reshape(1, sources.shape[0], combos, rows_here, 2, vectors * vectors)


def solution(mesh):
    placed = (
        P("tpair", None, None, None, "space"),
        P(),
        P("tpair", None, None, None, None),
        P(),
        P(),
    )
    return jax.shard_map(
        on_device,
        mesh=mesh,
        in_specs=placed,
        out_specs=P("tpair", None, None, "space", None, None),
        check_vma=False,
    )
```

```python
import functools

import jax
import jax.numpy as jnp
from jax import lax
from jax.experimental import pallas as pl
from jax.experimental.pallas import tpu as pltpu
from jax.sharding import PartitionSpec as P

LEXT = 64
TWO_PI = 6.283185307179586
LANES = 128
NT_DIMS = (((1,), (1,)), ((), ()))
NN_DIMS = (((1,), (0,)), ((), ()))


def elemental_kernel(place_ref, mom_ref, *refs, first, stride, parts, owners, sites_here, has_sum, last):
    inputs = refs[:parts]
    sum_ref = refs[parts] if has_sum else None
    refs = refs[parts + has_sum :]
    out_ref, v_ref, sem, vd_ref, p_ref, x0_ref, x1_ref = refs[:7]
    acc_ref, up_ref, low_ref = refs[7:] if last else (out_ref, None, None)
    vectors = v_ref.shape[3]
    half = vectors // 2
    rows = x0_ref.shape[0]
    per_chunk = rows // vectors
    chunks = half // per_chunk
    per_owner = sites_here // LANES
    blocks = v_ref.shape[0]

    copies = []
    for block in range(blocks):
        owner = block // per_owner
        ref = inputs[owner] if parts > 1 or owners == 1 else inputs[0].at[owner]
        at = block % per_owner * LANES
        copies.append(
            pltpu.make_async_copy(ref.at[:, :, :, at : at + LANES], v_ref.at[block], sem.at[block])
        )
    for copy in copies:
        copy.start()

    if has_sum and last:
        acc_ref[...] = sum_ref[...]
    elif not has_sum:
        acc_ref[...] = jnp.zeros_like(acc_ref)

    x1_ref[...] = jnp.zeros_like(x1_ref)
    p_ref[1] = jnp.zeros_like(p_ref[1])
    for copy in copies:
        copy.wait()
    lane = lax.broadcasted_iota(jnp.int32, (LANES, 2 * vectors), 1)
    total = place_ref[2]
    row = place_ref[1]
    factor = lax.rsqrt(jnp.full((1, LANES), 24.0, jnp.float32) * total.astype(jnp.float32))

    def one_block(block, unused):
        slot = block % 2
        owner = jnp.bitwise_xor(place_ref[0], first + stride * (block // per_owner))
        sites = (
            owner * sites_here
            + block % per_owner * LANES
            + lax.broadcasted_iota(jnp.int32, (1, LANES), 1)
        )
        turns = (
            mom_ref[row, 0] * jnp.bitwise_and(sites, LEXT - 1)
            + mom_ref[row, 1] * jnp.bitwise_and(sites // LEXT, LEXT - 1)
            + mom_ref[row, 2] * (sites // (LEXT * LEXT))
        )
        turns = jnp.bitwise_and(turns, LEXT - 1)
        angle = turns.astype(jnp.float32) * (TWO_PI / LEXT)
        cosine = jnp.cos(angle) * factor
        sine = jnp.sin(angle) * factor
        for colour in range(3):
            real = v_ref[block, 0, colour].astype(jnp.float32)
            imag = v_ref[block, 1, colour].astype(jnp.float32)
            for place, value in enumerate((real, imag, real + imag)):
                vd_ref[3 * place + colour, 0:vectors, :] = value
                vd_ref[3 * place + colour, vectors : 2 * vectors, :] = value
            p_real = cosine * real + sine * imag
            p_imag = cosine * imag - sine * real
            plain = jnp.transpose(jnp.concatenate([p_real, p_imag], axis=0))
            turned = pltpu.roll(plain, vectors, 1)
            signed = jnp.where(lane < vectors, plain, -plain)
            at = 2 * LANES * colour
            p_ref[slot, at : at + LANES, 0 : 2 * vectors] = signed.astype(jnp.bfloat16)
            p_ref[slot, at : at + LANES, 2 * vectors : 4 * vectors] = turned.astype(jnp.bfloat16)
            p_ref[slot, at + LANES : at + 2 * LANES, 0 : 2 * vectors] = (-turned).astype(
                jnp.bfloat16
            )
            p_ref[slot, at + LANES : at + 2 * LANES, 2 * vectors : 4 * vectors] = signed.astype(
                jnp.bfloat16
            )

        def cross(index, x_ref):
            for u in range(per_chunk):
                shift = index * per_chunk + u + 1
                for block in range(vectors // 16):
                    at_row = u * vectors + 16 * block
                    for colour in range(3):
                        up = (colour + 1) % 3
                        down = (colour + 2) % 3
                        reals = []
                        imags = []
                        for part in range(2):
                            row = 16 * block + 8 * part
                            parts = []
                            for place in range(3):
                                a_up = vd_ref[3 * place + up, row : row + 8, :]
                                a_down = vd_ref[3 * place + down, row : row + 8, :]
                                b_up = vd_ref[3 * place + up, pl.ds(shift + row, 8), :]
                                b_down = vd_ref[3 * place + down, pl.ds(shift + row, 8), :]
                                parts.append(a_up * b_down - a_down * b_up)
                            one, two, three = parts
                            reals.append(one - two)
                            imags.append(three - (one + two))
                        at = 2 * LANES * colour
                        x_ref[at_row : at_row + 16, at : at + LANES] = jnp.concatenate(
                            reals, axis=0
                        ).astype(jnp.bfloat16)
                        x_ref[at_row : at_row + 16, at + LANES : at + 2 * LANES] = jnp.concatenate(
                            imags, axis=0
                        ).astype(jnp.bfloat16)

        def add(index, x_ref, which):
            start = pl.multiple_of(index * rows, rows)
            acc_ref[pl.ds(start, rows), :] += lax.dot_general(
                x_ref[...], p_ref[which], NN_DIMS, preferred_element_type=jnp.float32
            )

        def two_chunks(index, carry):
            before = (2 * index + chunks - 1) % chunks
            cross(2 * index, x0_ref)
            add(before, x1_ref, jnp.where(index == 0, 1 - slot, slot))
            cross(2 * index + 1, x1_ref)
            add(2 * index, x0_ref, slot)
            return carry

        lax.fori_loop(0, chunks // 2, two_chunks, 0)
        return unused

    lax.fori_loop(0, blocks, one_block, 0)
    final = (blocks - 1) % 2
    start = (chunks - 1) * rows
    acc_ref[start : start + rows, :] += lax.dot_general(
        x1_ref[...], p_ref[final], NN_DIMS, preferred_element_type=jnp.float32
    )

    if last:

        def spread(index, carry):
            shift = index + 1
            for block in range(vectors // 8):
                start = pl.multiple_of(index * vectors + 8 * block, 8)
                for part in range(2):
                    value = acc_ref[pl.ds(start, 8), part * LANES : (part + 1) * LANES]
                    up_ref[part, pl.ds(8 * block * (2 * vectors + 1) + shift, 8, 2 * vectors + 1), :] = value
                    low_ref[
                        part, pl.ds(8 * block * (vectors + 1) + shift * vectors, 8, vectors + 1), :
                    ] = value
            return carry

        lax.fori_loop(0, half, spread, 0, unroll=4)

        def fold(j, carry):
            k = lax.broadcasted_iota(jnp.int32, (vectors, LANES), 0)
            wide = pl.multiple_of(j * 2 * vectors, vectors)
            narrow = pl.multiple_of(j * vectors, vectors)
            for part in range(2):
                near_up = up_ref[part, pl.ds(wide, vectors), :]
                far_up = up_ref[part, pl.ds(wide + vectors, vectors), :]
                near_low = low_ref[part, pl.ds(narrow, vectors), :]
                far_low = low_ref[part, pl.ds(narrow + vectors * vectors, vectors), :]
                above = jnp.where(k - j <= half, near_up, -far_low)
                below = jnp.where(j - k < half, -near_low, far_up)
                full = jnp.where(k > j, above, jnp.where(k < j, below, 0.0))
                out_ref[part, j] = full.astype(jnp.bfloat16)
            return carry

        lax.fori_loop(0, vectors, fold, 0, unroll=4)


def elementals(inputs, place, momenta, owners, first, stride, running, last):
    vectors, sites_here = inputs[0].shape[-2:]
    half = vectors // 2
    per_chunk = half // 2
    parts = len(inputs)
    blocks = (parts if owners == 1 else owners) * sites_here // LANES
    sum_shape = (half * vectors, 4 * vectors)
    vmem = pl.BlockSpec(memory_space=pltpu.VMEM)
    smem = pl.BlockSpec(memory_space=pltpu.SMEM)
    has_sum = running is not None
    scratch = [
        pltpu.VMEM((blocks, 2, 3, vectors, LANES), jnp.bfloat16),
        pltpu.SemaphoreType.DMA((blocks,)),
        pltpu.VMEM((9, 2 * vectors, LANES), jnp.float32),
        pltpu.VMEM((2, 6 * LANES, 4 * vectors), jnp.bfloat16),
        pltpu.VMEM((per_chunk * vectors, 6 * LANES), jnp.bfloat16),
        pltpu.VMEM((per_chunk * vectors, 6 * LANES), jnp.bfloat16),
    ]
    if last:
        out_shape = jax.ShapeDtypeStruct((2, vectors, vectors, 2 * vectors), jnp.bfloat16)
        scratch += [
            pltpu.VMEM(sum_shape, jnp.float32),
            pltpu.VMEM((2, 2 * vectors * vectors, LANES), jnp.float32),
            pltpu.VMEM((2, 2 * vectors * vectors, LANES), jnp.float32),
        ]
    else:
        out_shape = jax.ShapeDtypeStruct(sum_shape, jnp.float32)
    return pl.pallas_call(
        functools.partial(
            elemental_kernel,
            first=first,
            stride=stride,
            parts=parts,
            owners=owners,
            sites_here=sites_here,
            has_sum=has_sum,
            last=last,
        ),
        in_specs=[smem, smem] + [pl.BlockSpec(memory_space=pltpu.HBM)] * parts + [vmem] * has_sum,
        out_specs=vmem,
        out_shape=out_shape,
        scratch_shapes=scratch,
        input_output_aliases={2 + parts: 0} if has_sum and not last else {},
        compiler_params=pltpu.CompilerParams(
            vmem_limit_bytes=(40 if last else 12) << 20
        ),
        cost_estimate=pl.CostEstimate(
            flops=blocks * 2 * half * vectors * 6 * LANES * 4 * vectors,
            transcendentals=0,
            bytes_accessed=blocks * 6 * vectors * LANES * 2,
        ),
        name="elementals",
    )(place, momenta, *inputs, *([running] if has_sum else []))


def select_kernel(sources_ref, spins_ref, tau_ref, out_ref):
    combos, quarks, _ = spins_ref.shape
    for s in range(sources_ref.shape[0]):
        for n in range(combos):
            for q in range(quarks):
                code = spins_ref[n, q, 0] * 4 + spins_ref[n, q, 1]
                out_ref[s * combos + n, q] = tau_ref[sources_ref[s], code]


def select(tau, sources, spins):
    smem = pl.BlockSpec(memory_space=pltpu.SMEM)
    vmem = pl.BlockSpec(memory_space=pltpu.VMEM)
    return pl.pallas_call(
        select_kernel,
        in_specs=[smem, smem, vmem],
        out_specs=vmem,
        out_shape=jax.ShapeDtypeStruct(
            (sources.shape[0] * spins.shape[0], spins.shape[1]) + tau.shape[2:], tau.dtype
        ),
        compiler_params=pltpu.CompilerParams(vmem_limit_bytes=4 << 20),
        name="select",
    )(sources, spins, tau)


def baryon_kernel(
    info_ref, e_ref, tau_ref, out_ref, d_ref, m_ref, l0_ref, t_ref, w2_ref
):
    step = pl.program_id(0)
    vectors = e_ref.shape[1]
    count_sc = pl.num_programs(0)
    half = vectors // 2
    count = l0_ref.shape[0]
    rows_here = count // count_sc
    pitch = vectors + 1

    def block(at, q, part):
        return tau_ref[at, q, part].astype(jnp.float32)

    def flipped(at, q):
        return jnp.transpose(jnp.concatenate([block(at, q, 0), block(at, q, 1)], axis=0))[:vectors]

    @pl.when(step == 0)
    def _():
        for at in range(tau_ref.shape[0]):
            t_ref[...] = flipped(at, 0)
            l0_ref[at * rows_here : (at + 1) * rows_here] = t_ref[pl.ds(info_ref[3], rows_here), :]
        w2_ref[...] = jnp.zeros_like(w2_ref)
        left = l0_ref[...].astype(jnp.bfloat16)

        def one(pair, carry):
            right = jnp.concatenate(
                [e_ref[part, 2 * pair + side] for side in range(2) for part in range(2)], axis=0
            )
            value = lax.dot_general(left, right, NT_DIMS, preferred_element_type=jnp.float32)
            for side in range(2):
                for row in range(count // 8):
                    d_ref[pl.ds(8 * row * pitch + 2 * pair + side, 8, pitch), :] = value[
                        8 * row : 8 * row + 8, side * 2 * vectors : (side + 1) * 2 * vectors
                    ]
            return carry

        lax.fori_loop(0, half, one, 0, unroll=8)

    t_ref[...] = flipped(step, 1)
    left1 = jnp.concatenate(
        [t_ref[pl.ds(low, half, 2), :] for low in range(2)], axis=0
    ).astype(jnp.bfloat16)
    real = block(step, 2, 0)
    imag = block(step, 2, 1)
    quarters = ((real, imag), (-imag, real))
    for part in range(2):
        for q in range(2):
            piece = quarters[part][q]
            for low in range(2):
                rows = (2 * low + part) * vectors
                w2_ref[rows : rows + vectors, 2 * q * vectors : 2 * (q + 1) * vectors] = (
                    pltpu.roll(piece, low * vectors, 1) if low else piece
                ).astype(jnp.bfloat16)

    lanes = lax.broadcasted_iota(jnp.int32, (vectors, 2 * vectors), 1)
    signs = jnp.where(lanes < vectors, -1.0, 1.0).astype(jnp.bfloat16)
    group = 8

    def rows(index, carry):
        for pair in range(group // 2):
            columns = []
            for one in range(2):
                row = (step * rows_here + index * group + 2 * pair + one) * pitch
                plain = d_ref[pl.ds(row, vectors), :].astype(jnp.bfloat16)
                turned = pltpu.roll(plain, vectors, 1) * signs
                columns.append(jnp.concatenate([plain, turned], axis=0))
            right = jnp.concatenate(columns, axis=1)
            middle = lax.dot_general(left1, right, NN_DIMS, preferred_element_type=jnp.float32)
            middle = middle.astype(jnp.bfloat16)
            for one in range(2):
                at = one * 2 * vectors
                base = pl.multiple_of(index * group * half, group * half) + (2 * pair + one) * half
                m_ref[pl.ds(base, half), 0 : 2 * vectors] = middle[:half, at : at + 2 * vectors]
                m_ref[pl.ds(base, half), 2 * vectors :] = middle[half:, at : at + 2 * vectors]
        return carry

    lax.fori_loop(0, rows_here // group, rows, 0, unroll=min(8, rows_here // group))
    value = lax.dot_general(m_ref[...], w2_ref[...], NN_DIMS, preferred_element_type=jnp.float32)
    for part in range(2):
        out_ref[0, pl.ds(part, rows_here * half, 2), :] = value[
            :, part * 2 * vectors : (part + 1) * 2 * vectors
        ]


def baryons(elemental, tau, info, rows_here):
    vectors = elemental.shape[1]
    count_sc = tau.shape[0]
    vmem = pl.BlockSpec(memory_space=pltpu.VMEM)
    smem = pl.BlockSpec(memory_space=pltpu.SMEM)
    return pl.pallas_call(
        baryon_kernel,
        grid=(count_sc,),
        in_specs=[smem, vmem, vmem],
        out_specs=pl.BlockSpec((1, rows_here * vectors, 2 * vectors), lambda s: (s, 0, 0)),
        out_shape=jax.ShapeDtypeStruct(
            (count_sc, rows_here * vectors, 2 * vectors), jnp.float32
        ),
        scratch_shapes=[
            pltpu.VMEM((count_sc * rows_here * (vectors + 1), 2 * vectors), jnp.float32),
            pltpu.VMEM((rows_here * vectors // 2, 4 * vectors), jnp.bfloat16),
            pltpu.VMEM((count_sc * rows_here, 2 * vectors), jnp.float32),
            pltpu.VMEM((vectors, 2 * vectors), jnp.float32),
            pltpu.VMEM((4 * vectors, 4 * vectors), jnp.bfloat16),
        ],
        compiler_params=pltpu.CompilerParams(
            dimension_semantics=("arbitrary",), vmem_limit_bytes=40 << 20
        ),
        name="baryons",
    )(info, elemental, tau)


def on_device(eigvecs, momenta, perams, sources, spins):
    vecs = eigvecs[0]
    vectors, sites_here = vecs.shape[2:]
    mom_count = momenta.shape[0]
    combos = spins.shape[0]
    space_count = lax.axis_size("space")
    place = lax.axis_index("space")
    rows_here = mom_count * vectors // space_count
    count_sc = sources.shape[0] * combos
    if vectors % rows_here or sites_here % LANES:
        raise ValueError("sizes")
    own_momentum = place * rows_here // vectors

    tau = lax.all_to_all(perams[0], "tpair", split_axis=0, concat_axis=0, tiled=True)

    by_permute = space_count == 8
    info = jnp.stack(
        [
            place if by_permute else 0 * place,
            own_momentum,
            0 * place + sites_here * space_count,
            place * rows_here % vectors,
        ]
    ).astype(jnp.int32)
    if by_permute:

        def swap(value, distance):
            return lax.ppermute(
                value, "space", [(n, n ^ distance) for n in range(space_count)]
            )

        beside = swap(vecs, 1)
        along = [swap(vecs, distance) for distance in range(2, space_count, 2)]
        others = swap(jnp.stack(along), 1)
        running = elementals([vecs, beside], info, momenta, 1, 0, 1, None, False)
        running = elementals(along, info, momenta, 1, 2, 2, running, False)
        elemental = elementals(
            [others], info, momenta, len(along), 3, 2, running, True
        )
    else:
        gathered = lax.all_gather(vecs, "space", axis=0, tiled=False)
        elemental = elementals([gathered], info, momenta, space_count, 0, 1, None, True)

    tau = select(tau, sources, spins)
    tau = tau.reshape(tau.shape[:3] + (vectors, vectors))
    tau = jnp.pad(tau, ((0, 0),) * 4 + ((0, vectors),))
    result = baryons(elemental, tau, info, rows_here)
    result = result.reshape(count_sc, rows_here, vectors // 2, 2, 2 * vectors)
    result = jnp.transpose(result, (0, 1, 3, 2, 4))
    return result.reshape(1, sources.shape[0], combos, rows_here, 2, vectors * vectors)


def solution(mesh):
    placed = (
        P("tpair", None, None, None, "space"),
        P(),
        P("tpair", None, None, None, None),
        P(),
        P(),
    )
    return jax.shard_map(
        on_device,
        mesh=mesh,
        in_specs=placed,
        out_specs=P("tpair", None, None, "space", None, None),
        check_vma=False,
    )
```

```python
import functools

import jax
import jax.numpy as jnp
from jax import lax
from jax.experimental import pallas as pl
from jax.experimental.pallas import tpu as pltpu
from jax.sharding import PartitionSpec as P

LEXT = 64
TWO_PI = 6.283185307179586
LANES = 128
NT_DIMS = (((1,), (1,)), ((), ()))
NN_DIMS = (((1,), (0,)), ((), ()))


def elemental_kernel(place_ref, mom_ref, *refs, first, stride, parts, owners, sites_here, has_sum, last):
    inputs = refs[:parts]
    sum_ref = refs[parts] if has_sum else None
    refs = refs[parts + has_sum :]
    out_ref, v_ref, sem, vd_ref, p_ref, x0_ref, x1_ref = refs[:7]
    acc_ref, up_ref, low_ref = refs[7:] if last else (out_ref, None, None)
    vectors = v_ref.shape[3]
    half = vectors // 2
    rows = x0_ref.shape[0]
    per_chunk = rows // vectors
    chunks = half // per_chunk
    per_owner = sites_here // LANES
    blocks = v_ref.shape[0]

    copies = []
    for block in range(blocks):
        owner = block // per_owner
        ref = inputs[owner] if parts > 1 or owners == 1 else inputs[0].at[owner]
        at = block % per_owner * LANES
        copies.append(
            pltpu.make_async_copy(ref.at[:, :, :, at : at + LANES], v_ref.at[block], sem.at[block])
        )
    for copy in copies:
        copy.start()

    if has_sum and last:
        acc_ref[...] = sum_ref[...]
    elif not has_sum:
        acc_ref[...] = jnp.zeros_like(acc_ref)

    x1_ref[...] = jnp.zeros_like(x1_ref)
    p_ref[1] = jnp.zeros_like(p_ref[1])
    for copy in copies:
        copy.wait()
    lane = lax.broadcasted_iota(jnp.int32, (LANES, 2 * vectors), 1)
    total = place_ref[2]
    row = place_ref[1]
    factor = lax.rsqrt(jnp.full((1, LANES), 24.0, jnp.float32) * total.astype(jnp.float32))

    def one_block(block, unused):
        slot = block % 2
        owner = jnp.bitwise_xor(place_ref[0], first + stride * (block // per_owner))
        sites = (
            owner * sites_here
            + block % per_owner * LANES
            + lax.broadcasted_iota(jnp.int32, (1, LANES), 1)
        )
        turns = (
            mom_ref[row, 0] * jnp.bitwise_and(sites, LEXT - 1)
            + mom_ref[row, 1] * jnp.bitwise_and(sites // LEXT, LEXT - 1)
            + mom_ref[row, 2] * (sites // (LEXT * LEXT))
        )
        turns = jnp.bitwise_and(turns, LEXT - 1)
        angle = turns.astype(jnp.float32) * (TWO_PI / LEXT)
        cosine = jnp.cos(angle) * factor
        sine = jnp.sin(angle) * factor
        for colour in range(3):
            real = v_ref[block, 0, colour].astype(jnp.float32)
            imag = v_ref[block, 1, colour].astype(jnp.float32)
            for place, value in enumerate((real, imag, real + imag)):
                vd_ref[3 * place + colour, 0:vectors, :] = value
                vd_ref[3 * place + colour, vectors : 2 * vectors, :] = value
            p_real = cosine * real + sine * imag
            p_imag = cosine * imag - sine * real
            plain = jnp.transpose(jnp.concatenate([p_real, p_imag], axis=0))
            turned = pltpu.roll(plain, vectors, 1)
            signed = jnp.where(lane < vectors, plain, -plain)
            at = 2 * LANES * colour
            p_ref[slot, at : at + LANES, 0 : 2 * vectors] = signed.astype(jnp.bfloat16)
            p_ref[slot, at : at + LANES, 2 * vectors : 4 * vectors] = turned.astype(jnp.bfloat16)
            p_ref[slot, at + LANES : at + 2 * LANES, 0 : 2 * vectors] = (-turned).astype(
                jnp.bfloat16
            )
            p_ref[slot, at + LANES : at + 2 * LANES, 2 * vectors : 4 * vectors] = signed.astype(
                jnp.bfloat16
            )

        def cross(index, x_ref):
            for u in range(per_chunk):
                shift = index * per_chunk + u + 1
                for block in range(vectors // 16):
                    at_row = u * vectors + 16 * block
                    for colour in range(3):
                        up = (colour + 1) % 3
                        down = (colour + 2) % 3
                        reals = []
                        imags = []
                        for part in range(2):
                            row = 16 * block + 8 * part
                            parts = []
                            for place in range(3):
                                a_up = vd_ref[3 * place + up, row : row + 8, :]
                                a_down = vd_ref[3 * place + down, row : row + 8, :]
                                b_up = vd_ref[3 * place + up, pl.ds(shift + row, 8), :]
                                b_down = vd_ref[3 * place + down, pl.ds(shift + row, 8), :]
                                parts.append(a_up * b_down - a_down * b_up)
                            one, two, three = parts
                            reals.append(one - two)
                            imags.append(three - (one + two))
                        at = 2 * LANES * colour
                        x_ref[at_row : at_row + 16, at : at + LANES] = jnp.concatenate(
                            reals, axis=0
                        ).astype(jnp.bfloat16)
                        x_ref[at_row : at_row + 16, at + LANES : at + 2 * LANES] = jnp.concatenate(
                            imags, axis=0
                        ).astype(jnp.bfloat16)

        def add(index, x_ref, which):
            start = pl.multiple_of(index * rows, rows)
            acc_ref[pl.ds(start, rows), :] += lax.dot_general(
                x_ref[...], p_ref[which], NN_DIMS, preferred_element_type=jnp.float32
            )

        def two_chunks(index, carry):
            before = (2 * index + chunks - 1) % chunks
            cross(2 * index, x0_ref)
            add(before, x1_ref, jnp.where(index == 0, 1 - slot, slot))
            cross(2 * index + 1, x1_ref)
            add(2 * index, x0_ref, slot)
            return carry

        lax.fori_loop(0, chunks // 2, two_chunks, 0)
        return unused

    lax.fori_loop(0, blocks, one_block, 0)
    final = (blocks - 1) % 2
    start = (chunks - 1) * rows
    acc_ref[start : start + rows, :] += lax.dot_general(
        x1_ref[...], p_ref[final], NN_DIMS, preferred_element_type=jnp.float32
    )

    if last:

        def spread(index, carry):
            shift = index + 1
            for block in range(vectors // 8):
                start = pl.multiple_of(index * vectors + 8 * block, 8)
                for part in range(2):
                    value = acc_ref[pl.ds(start, 8), part * LANES : (part + 1) * LANES]
                    up_ref[part, pl.ds(8 * block * (2 * vectors + 1) + shift, 8, 2 * vectors + 1), :] = value
                    low_ref[
                        part, pl.ds(8 * block * (vectors + 1) + shift * vectors, 8, vectors + 1), :
                    ] = value
            return carry

        lax.fori_loop(0, half, spread, 0, unroll=4)

        def fold(j, carry):
            k = lax.broadcasted_iota(jnp.int32, (vectors, LANES), 0)
            wide = pl.multiple_of(j * 2 * vectors, vectors)
            narrow = pl.multiple_of(j * vectors, vectors)
            for part in range(2):
                near_up = up_ref[part, pl.ds(wide, vectors), :]
                far_up = up_ref[part, pl.ds(wide + vectors, vectors), :]
                near_low = low_ref[part, pl.ds(narrow, vectors), :]
                far_low = low_ref[part, pl.ds(narrow + vectors * vectors, vectors), :]
                above = jnp.where(k - j <= half, near_up, -far_low)
                below = jnp.where(j - k < half, -near_low, far_up)
                full = jnp.where(k > j, above, jnp.where(k < j, below, 0.0))
                out_ref[part, j] = full.astype(jnp.bfloat16)
            return carry

        lax.fori_loop(0, vectors, fold, 0, unroll=4)


def elementals(inputs, place, momenta, owners, first, stride, running, last):
    vectors, sites_here = inputs[0].shape[-2:]
    half = vectors // 2
    per_chunk = half // 2
    parts = len(inputs)
    blocks = (parts if owners == 1 else owners) * sites_here // LANES
    sum_shape = (half * vectors, 4 * vectors)
    vmem = pl.BlockSpec(memory_space=pltpu.VMEM)
    smem = pl.BlockSpec(memory_space=pltpu.SMEM)
    has_sum = running is not None
    scratch = [
        pltpu.VMEM((blocks, 2, 3, vectors, LANES), jnp.bfloat16),
        pltpu.SemaphoreType.DMA((blocks,)),
        pltpu.VMEM((9, 2 * vectors, LANES), jnp.float32),
        pltpu.VMEM((2, 6 * LANES, 4 * vectors), jnp.bfloat16),
        pltpu.VMEM((per_chunk * vectors, 6 * LANES), jnp.bfloat16),
        pltpu.VMEM((per_chunk * vectors, 6 * LANES), jnp.bfloat16),
    ]
    if last:
        out_shape = jax.ShapeDtypeStruct((2, vectors, vectors, 2 * vectors), jnp.bfloat16)
        scratch += [
            pltpu.VMEM(sum_shape, jnp.float32),
            pltpu.VMEM((2, 2 * vectors * vectors, LANES), jnp.float32),
            pltpu.VMEM((2, 2 * vectors * vectors, LANES), jnp.float32),
        ]
    else:
        out_shape = jax.ShapeDtypeStruct(sum_shape, jnp.float32)
    return pl.pallas_call(
        functools.partial(
            elemental_kernel,
            first=first,
            stride=stride,
            parts=parts,
            owners=owners,
            sites_here=sites_here,
            has_sum=has_sum,
            last=last,
        ),
        in_specs=[smem, smem] + [pl.BlockSpec(memory_space=pltpu.HBM)] * parts + [vmem] * has_sum,
        out_specs=vmem,
        out_shape=out_shape,
        scratch_shapes=scratch,
        input_output_aliases={2 + parts: 0} if has_sum and not last else {},
        compiler_params=pltpu.CompilerParams(
            vmem_limit_bytes=(40 if last else 12) << 20
        ),
        cost_estimate=pl.CostEstimate(
            flops=blocks * 2 * half * vectors * 6 * LANES * 4 * vectors,
            transcendentals=0,
            bytes_accessed=blocks * 6 * vectors * LANES * 2,
        ),
        name="elementals",
    )(place, momenta, *inputs, *([running] if has_sum else []))


def select_kernel(sources_ref, spins_ref, tau_ref, out_ref):
    combos, quarks, _ = spins_ref.shape
    for s in range(sources_ref.shape[0]):
        for n in range(combos):
            for q in range(quarks):
                code = spins_ref[n, q, 0] * 4 + spins_ref[n, q, 1]
                out_ref[s * combos + n, q] = tau_ref[sources_ref[s], code]


def select(tau, sources, spins):
    smem = pl.BlockSpec(memory_space=pltpu.SMEM)
    vmem = pl.BlockSpec(memory_space=pltpu.VMEM)
    return pl.pallas_call(
        select_kernel,
        in_specs=[smem, smem, vmem],
        out_specs=vmem,
        out_shape=jax.ShapeDtypeStruct(
            (sources.shape[0] * spins.shape[0], spins.shape[1]) + tau.shape[2:], tau.dtype
        ),
        compiler_params=pltpu.CompilerParams(vmem_limit_bytes=4 << 20),
        name="select",
    )(sources, spins, tau)


def baryon_kernel(
    info_ref, e_ref, tau_ref, out_ref, d_ref, m_ref, l0_ref, t_ref, w2_ref
):
    step = pl.program_id(0)
    vectors = e_ref.shape[1]
    count_sc = pl.num_programs(0)
    half = vectors // 2
    count = l0_ref.shape[0]
    rows_here = count // count_sc
    pitch = vectors + 1

    def block(at, q, part):
        return tau_ref[at, q, part].astype(jnp.float32)

    def flipped(at, q):
        return jnp.transpose(jnp.concatenate([block(at, q, 0), block(at, q, 1)], axis=0))[:vectors]

    @pl.when(step == 0)
    def _():
        for at in range(tau_ref.shape[0]):
            t_ref[...] = flipped(at, 0)
            l0_ref[at * rows_here : (at + 1) * rows_here] = t_ref[pl.ds(info_ref[3], rows_here), :]
        w2_ref[...] = jnp.zeros_like(w2_ref)
        left = l0_ref[...].astype(jnp.bfloat16)

        def one(pair, carry):
            right = jnp.concatenate(
                [e_ref[part, 2 * pair + side] for side in range(2) for part in range(2)], axis=0
            )
            value = lax.dot_general(left, right, NT_DIMS, preferred_element_type=jnp.float32)
            for side in range(2):
                for row in range(count // 8):
                    d_ref[pl.ds(8 * row * pitch + 2 * pair + side, 8, pitch), :] = value[
                        8 * row : 8 * row + 8, side * 2 * vectors : (side + 1) * 2 * vectors
                    ]
            return carry

        lax.fori_loop(0, half, one, 0, unroll=8)

    t_ref[...] = flipped(step, 1)
    left1 = jnp.concatenate(
        [t_ref[pl.ds(low, half, 2), :] for low in range(2)], axis=0
    ).astype(jnp.bfloat16)
    real = block(step, 2, 0)
    imag = block(step, 2, 1)
    quarters = ((real, imag), (-imag, real))
    for part in range(2):
        for q in range(2):
            piece = quarters[part][q]
            for low in range(2):
                rows = (2 * low + part) * vectors
                w2_ref[rows : rows + vectors, 2 * q * vectors : 2 * (q + 1) * vectors] = (
                    pltpu.roll(piece, low * vectors, 1) if low else piece
                ).astype(jnp.bfloat16)

    lanes = lax.broadcasted_iota(jnp.int32, (vectors, 2 * vectors), 1)
    signs = jnp.where(lanes < vectors, -1.0, 1.0).astype(jnp.bfloat16)
    group = 8

    def rows(index, carry):
        for pair in range(group // 2):
            columns = []
            for one in range(2):
                row = (step * rows_here + index * group + 2 * pair + one) * pitch
                plain = d_ref[pl.ds(row, vectors), :].astype(jnp.bfloat16)
                turned = pltpu.roll(plain, vectors, 1) * signs
                columns.append(jnp.concatenate([plain, turned], axis=0))
            right = jnp.concatenate(columns, axis=1)
            middle = lax.dot_general(left1, right, NN_DIMS, preferred_element_type=jnp.float32)
            middle = middle.astype(jnp.bfloat16)
            for one in range(2):
                at = one * 2 * vectors
                base = pl.multiple_of(index * group * half, group * half) + (2 * pair + one) * half
                m_ref[pl.ds(base, half), 0 : 2 * vectors] = middle[:half, at : at + 2 * vectors]
                m_ref[pl.ds(base, half), 2 * vectors :] = middle[half:, at : at + 2 * vectors]
        return carry

    lax.fori_loop(0, rows_here // group, rows, 0, unroll=min(8, rows_here // group))
    value = lax.dot_general(m_ref[...], w2_ref[...], NN_DIMS, preferred_element_type=jnp.float32)
    for part in range(2):
        out_ref[0, pl.ds(part, rows_here * half, 2), :] = value[
            :, part * 2 * vectors : (part + 1) * 2 * vectors
        ]


def baryons(elemental, tau, info, rows_here):
    vectors = elemental.shape[1]
    count_sc = tau.shape[0]
    vmem = pl.BlockSpec(memory_space=pltpu.VMEM)
    smem = pl.BlockSpec(memory_space=pltpu.SMEM)
    return pl.pallas_call(
        baryon_kernel,
        grid=(count_sc,),
        in_specs=[smem, vmem, vmem],
        out_specs=pl.BlockSpec((1, rows_here * vectors, 2 * vectors), lambda s: (s, 0, 0)),
        out_shape=jax.ShapeDtypeStruct(
            (count_sc, rows_here * vectors, 2 * vectors), jnp.float32
        ),
        scratch_shapes=[
            pltpu.VMEM((count_sc * rows_here * (vectors + 1), 2 * vectors), jnp.float32),
            pltpu.VMEM((rows_here * vectors // 2, 4 * vectors), jnp.bfloat16),
            pltpu.VMEM((count_sc * rows_here, 2 * vectors), jnp.float32),
            pltpu.VMEM((vectors, 2 * vectors), jnp.float32),
            pltpu.VMEM((4 * vectors, 4 * vectors), jnp.bfloat16),
        ],
        compiler_params=pltpu.CompilerParams(
            dimension_semantics=("arbitrary",), vmem_limit_bytes=40 << 20
        ),
        name="baryons",
    )(info, elemental, tau)


def on_device(eigvecs, momenta, perams, sources, spins):
    vecs = eigvecs[0]
    vectors, sites_here = vecs.shape[2:]
    mom_count = momenta.shape[0]
    combos = spins.shape[0]
    space_count = lax.axis_size("space")
    place = lax.axis_index("space")
    rows_here = mom_count * vectors // space_count
    count_sc = sources.shape[0] * combos
    if vectors % rows_here or sites_here % LANES:
        raise ValueError("sizes")
    own_momentum = place * rows_here // vectors

    tau = lax.all_to_all(perams[0], "tpair", split_axis=0, concat_axis=0, tiled=True)

    by_permute = space_count == 8
    info = jnp.stack(
        [
            place if by_permute else 0 * place,
            own_momentum,
            0 * place + sites_here * space_count,
            place * rows_here % vectors,
        ]
    ).astype(jnp.int32)
    if by_permute:

        def swap(value, distance):
            return lax.ppermute(
                value, "space", [(n, n ^ distance) for n in range(space_count)]
            )

        beside = swap(vecs, 1)
        along = [swap(vecs, distance) for distance in range(2, space_count, 2)]
        others = swap(jnp.stack(along), 1)
        running = elementals([vecs], info, momenta, 1, 0, 1, None, False)
        running = elementals([beside], info, momenta, 1, 1, 1, running, False)
        running = elementals(along, info, momenta, 1, 2, 2, running, False)
        elemental = elementals(
            [others], info, momenta, len(along), 3, 2, running, True
        )
    else:
        gathered = lax.all_gather(vecs, "space", axis=0, tiled=False)
        elemental = elementals([gathered], info, momenta, space_count, 0, 1, None, True)

    tau = select(tau, sources, spins)
    tau = tau.reshape(tau.shape[:3] + (vectors, vectors))
    tau = jnp.pad(tau, ((0, 0),) * 4 + ((0, vectors),))
    result = baryons(elemental, tau, info, rows_here)
    result = result.reshape(count_sc, rows_here, vectors // 2, 2, 2 * vectors)
    result = jnp.transpose(result, (0, 1, 3, 2, 4))
    return result.reshape(1, sources.shape[0], combos, rows_here, 2, vectors * vectors)


def solution(mesh):
    placed = (
        P("tpair", None, None, None, "space"),
        P(),
        P("tpair", None, None, None, None),
        P(),
        P(),
    )
    return jax.shard_map(
        on_device,
        mesh=mesh,
        in_specs=placed,
        out_specs=P("tpair", None, None, "space", None, None),
        check_vma=False,
    )
```
